32 devices in a mesh: grp: 2 (over y), freq: 4 (over z), beam: 2 (over x), dm: 2 (over core).
Axes of the slice: x: 2, y: 2, z: 4, core: 2. Of those that a mesh axis runs over, the one named last changes fastest.
Arguments:
- voltages: bfloat16 [4, 2048, 16, 2, 1024], P(None, ('freq', 'beam'), ('grp', 'dm')), parts along dimension 2, may hold values from -6 to 6
- grid_feed: int32 [1024], replicated, may hold values from 0 to 1023, each once
- delays: int32 [4, 2048, 256], P('freq', None, 'dm'), may hold values from 0 to 4
Outputs:
- dedispersed: float32 [4, 256, 8, 1024], P('freq', 'dm', 'grp', 'beam'), parts along dimension 2
The draws below stay inside these ranges and needn't reach their ends.
There are 2 independent parts, one for each index of `grp`. The reference program is written for one: setup_inputs(seed, part) draws one part's arguments, and reference() takes and returns one part's arrays. A program takes and returns all parts, laid end to end along the dimension named above; an argument that names none is the same for every part. Nothing has to cross between parts.
Inputs may be any that keep to these rules, and one draw needn't show every extreme that they name: `grid_feed`: each feed appears once.
All inputs are finite; a program needn't handle non-finite values.
Results may differ from the reference program's by a relative error of at most 0.0034.
Values may be sent and summed in bfloat16 or wider, within the bound.
A program may use at most 128 MiB of HBM per device.

```python
import math
import jax
import jax.numpy as jnp
from jax import lax

GX = 4
GY = 256
FEEDS = 1024
FREQS = 8192
DMS = 256
TIME = 8
TOUT = 4
NBAND = 4
SUBS = 2048


def draw_delays(key, part):
    deepest = TIME - TOUT
    channels = NBAND * SUBS
    key_value, key_jitter, key_place = jax.random.split(jax.random.fold_in(key, 7), 3)
    position = jnp.arange(channels, dtype=jnp.int32)
    lowered = 2 * channels - position
    quotient = 4 * channels * channels // lowered
    weight = quotient * 1024 // lowered - 1024
    heaviest = jnp.max(weight)
    trial_value = jax.random.randint(key_value, (DMS,), 0, deepest + 1, dtype=jnp.int32)
    forced_dm = jax.random.randint(key_place, (), 0, DMS, dtype=jnp.int32)
    trial_value = jnp.where(jnp.arange(DMS, dtype=jnp.int32) == forced_dm, deepest, trial_value)
    base_delay = trial_value[None, :] * weight[:, None] // heaviest
    jitter = jax.random.randint(key_jitter, (channels, DMS), 0, 2, dtype=jnp.int32)
    return jnp.minimum(base_delay + jitter, deepest).reshape(NBAND, SUBS, DMS).astype(jnp.int32)


def shard_levels(stream_key, shape, cuts, smallest, top_value):
    def one(dim, shards_of):
        heights = jax.random.uniform(jax.random.fold_in(jax.random.fold_in(stream_key, 6), dim), (shards_of,), jnp.float32, smallest / len(cuts), top_value / len(cuts))
        return jnp.repeat(jnp.exp(heights), shape[dim] // shards_of).reshape((-1,) + (1,) * (len(shape) - dim - 1))

    loudness = one(*cuts[0])
    for cut in cuts[1:]:
        loudness = loudness * one(*cut)
    return loudness


def gaussian(rng, shape, spread, bound, cuts=(), kind=jnp.bfloat16):
    loudness = shard_levels(rng, shape, cuts, -0.22, 0.18) if cuts else 1.0
    array = jax.random.normal(rng, shape, jnp.float32) * spread * loudness
    return jnp.minimum(jnp.maximum(array, -bound), bound).astype(kind)


def setup_inputs(seed: int = 0, part: int = 0) -> dict:
    key_list = jax.random.split(jax.random.key(seed), 4)
    part_splits = jax.random.split(jax.random.fold_in(key_list[3], part), 4)
    return {
        "voltages": gaussian(part_splits[0], (NBAND, SUBS, TIME, 2, FEEDS), 1.0, 6.0, ((1, 8), (2, 2))),
        "grid_feed": jax.random.permutation(key_list[1], FEEDS).astype(jnp.int32),
        "delays": draw_delays(jax.random.fold_in(key_list[3], 71), part),
    }


def steering_table(length, factor):
    position = jnp.arange(length, dtype=jnp.int32)
    phase_step = position[:, None] * position[None, :] % length
    phase_angle = phase_step.astype(jnp.float32) * (2.0 * math.pi / length)
    cosine = jnp.cos(phase_angle) * factor
    sine_part = jnp.sin(phase_angle) * factor
    upper_half = jnp.concatenate([cosine, -sine_part], axis=1)
    lower_half = jnp.concatenate([sine_part, cosine], axis=1)
    return jnp.concatenate([upper_half, lower_half], axis=0).astype(jnp.bfloat16)

def quarter_table():
    position = jnp.arange(GX, dtype=jnp.int32)
    phase_step = position[:, None] * position[None, :] % GX
    cosine = jnp.where(phase_step == 0, 1.0, jnp.where(phase_step == 2, -1.0, 0.0)) * 0.5
    sine_part = jnp.where(phase_step == 1, 1.0, jnp.where(phase_step == 3, -1.0, 0.0)) * 0.5
    real_in = jnp.stack([cosine, -sine_part], axis=2)
    imag_in = jnp.stack([sine_part, cosine], axis=2)
    return jnp.stack([real_in, imag_in], axis=1).astype(jnp.float32)

def form_power(voltages, grid_feed):
    row_count = voltages.shape[0] * voltages.shape[1] * voltages.shape[2]
    feed_count = voltages.shape[4]
    gridded = jnp.take(voltages.reshape(row_count, 2, feed_count), grid_feed, axis=2)
    gridded = jnp.transpose(gridded.reshape(row_count, 2, GX, GY), (0, 2, 1, 3)).reshape(row_count * GX, 2 * GY)
    along_y = jnp.dot(gridded, steering_table(GY, 1.0 / math.sqrt(GY)), preferred_element_type=jnp.float32).astype(jnp.bfloat16)
    along_y = along_y.reshape(row_count, GX, 2, GY).astype(jnp.float32)
    formed = jnp.einsum('rgpy,gpbq->rbqy', along_y, quarter_table(), precision=lax.Precision.HIGHEST)
    intensity = 0.5 * (formed[:, :, 0, :] ** 2 + formed[:, :, 1, :] ** 2)
    return intensity.astype(jnp.bfloat16).reshape(row_count, feed_count)

def reference(voltages, grid_feed, delays):
    band_count, sub_count, total_time = (voltages.shape[0], voltages.shape[1], voltages.shape[2])
    feed_count = voltages.shape[4]
    dm_count = delays.shape[2]
    intensity = form_power(voltages, grid_feed).reshape(band_count, sub_count, total_time, feed_count)
    levels = intensity.astype(jnp.float32)
    centered = (levels - lax.optimization_barrier(jnp.mean(levels, axis=2, keepdims=True))).astype(jnp.bfloat16)
    out_time = total_time // 2
    offsets = jnp.arange(out_time, dtype=jnp.int32)
    factor = 1.0 / math.sqrt(FREQS)

    def one_channel(running, entries):
        channel_rows, lag_row = entries
        picked = jnp.take(channel_rows, lag_row[:, None] + offsets[None, :], axis=0)
        return (running + picked.astype(jnp.float32), None)

    def one_band(cumulative, entries):
        band_rows, band_lags = entries
        initial = jnp.zeros((dm_count, out_time, feed_count), jnp.float32)
        band_sum, _ = lax.scan(one_channel, initial, (band_rows, band_lags))
        cumulative = cumulative + band_sum
        return (cumulative, cumulative * factor)
    zeros_start = jnp.zeros((dm_count, out_time, feed_count), jnp.float32)
    _, outputs = lax.scan(one_band, zeros_start, (centered, delays))
    return outputs
```

```python
import functools
import math

import jax
import jax.numpy as jnp
from jax import lax
from jax.experimental import pallas as pl
from jax.experimental.pallas import tpu as pltpu
from jax.sharding import PartitionSpec as P

GX = 4
GY = 256
FREQS = 8192
ROW_BLOCK = 256


def steering_table(length, factor):
    position = jnp.arange(length, dtype=jnp.int32)
    phase_step = position[:, None] * position[None, :] % length
    phase_angle = phase_step.astype(jnp.float32) * (2.0 * math.pi / length)
    cosine = jnp.cos(phase_angle) * factor
    sine_part = jnp.sin(phase_angle) * factor
    upper_half = jnp.concatenate([cosine, -sine_part], axis=1)
    lower_half = jnp.concatenate([sine_part, cosine], axis=1)
    return jnp.concatenate([upper_half, lower_half], axis=0).astype(jnp.bfloat16)


def quarter_table():
    position = jnp.arange(GX, dtype=jnp.int32)
    phase_step = position[:, None] * position[None, :] % GX
    cosine = jnp.where(phase_step == 0, 1.0, jnp.where(phase_step == 2, -1.0, 0.0)) * 0.5
    sine_part = jnp.where(phase_step == 1, 1.0, jnp.where(phase_step == 3, -1.0, 0.0)) * 0.5
    real_in = jnp.stack([cosine, -sine_part], axis=2)
    imag_in = jnp.stack([sine_part, cosine], axis=2)
    return jnp.stack([real_in, imag_in], axis=1).astype(jnp.float32)


def form_power(voltages, grid_feed):
    row_count = voltages.shape[0] * voltages.shape[1] * voltages.shape[2]
    feed_count = voltages.shape[4]
    gridded = jnp.take(voltages.reshape(row_count, 2, feed_count), grid_feed, axis=2)
    gridded = jnp.transpose(gridded.reshape(row_count, 2, GX, GY), (0, 2, 1, 3)).reshape(
        row_count * GX, 2 * GY
    )
    along_y = jnp.dot(
        gridded, steering_table(GY, 1.0 / math.sqrt(GY)), preferred_element_type=jnp.float32
    ).astype(jnp.bfloat16)
    along_y = along_y.reshape(row_count, GX, 2, GY).astype(jnp.float32)
    formed = jnp.einsum(
        "rgpy,gpbq->rbqy", along_y, quarter_table(), precision=lax.Precision.HIGHEST
    )
    intensity = 0.5 * (formed[:, :, 0, :] ** 2 + formed[:, :, 1, :] ** 2)
    return intensity.astype(jnp.bfloat16).reshape(row_count, feed_count)


def regrouped_body(voltages, grid_feed, delays):
    band_count, sub_local, time_local = (voltages.shape[0], voltages.shape[1], voltages.shape[2])
    feed_count = voltages.shape[4]
    columns = lax.axis_size("beam")
    col_width = feed_count // columns
    intensity = form_power(voltages, grid_feed).reshape(
        band_count, sub_local, time_local, columns, col_width
    )
    regrouped = jnp.transpose(intensity, (0, 3, 1, 2, 4)).reshape(
        band_count * columns, sub_local, time_local, col_width
    )
    turned = lax.all_to_all(regrouped, ("freq", "beam"), split_axis=0, concat_axis=1, tiled=True)
    turned = turned.reshape(-1, time_local, col_width)
    full_time = lax.all_gather(turned, "dm", axis=1, tiled=True)
    sub_count, total_time = (full_time.shape[0], full_time.shape[1])
    levels = full_time.astype(jnp.float32)
    centered = (levels - jnp.mean(levels, axis=1, keepdims=True)).astype(jnp.bfloat16)
    flattened = centered.reshape(sub_count * total_time, col_width)
    out_time = total_time // 2
    offsets = jnp.arange(out_time, dtype=jnp.int32)
    sample_ids = jnp.arange(total_time, dtype=jnp.int32)
    dm_local = delays.shape[2]
    dm_block = 32
    lag_blocks = jnp.transpose(delays[0]).reshape(dm_local // dm_block, dm_block, sub_count)

    def dedisperse(lag_rows):
        shifted = offsets[None, :, None] + lag_rows[:, None, :]
        selector = (shifted[:, :, :, None] == sample_ids[None, None, None, :]).astype(jnp.bfloat16)
        summed = jnp.dot(
            selector.reshape(dm_block * out_time, sub_count * total_time),
            flattened,
            preferred_element_type=jnp.float32,
        )
        return summed.reshape(dm_block, out_time, col_width)

    partial_sum = lax.map(dedisperse, lag_blocks).reshape(dm_local, out_time, col_width)
    cumulative = lax.all_to_all(
        jnp.cumsum(
            lax.all_to_all(partial_sum[None], "freq", split_axis=1, concat_axis=0, tiled=True),
            axis=0,
        ),
        "freq",
        split_axis=0,
        concat_axis=1,
        tiled=True,
    )
    return cumulative * (1.0 / math.sqrt(FREQS))


def beam_kernel(volt_ref, place_ref, table_ref, out_ref):
    planes = [
        jnp.dot(volt_ref[p], place_ref[...], preferred_element_type=jnp.float32).astype(
            jnp.bfloat16
        )
        for p in range(2)
    ]
    real, imag = [], []
    for g in range(GX):
        cells = jnp.concatenate([plane[:, g * GY : (g + 1) * GY] for plane in planes], axis=1)
        line = jnp.dot(cells, table_ref[...], preferred_element_type=jnp.float32)
        line = line.astype(jnp.bfloat16).astype(jnp.float32)
        real.append(line[:, :GY])
        imag.append(line[:, GY:])
    even_r, even_i = real[0] + real[2], imag[0] + imag[2]
    odd_r, odd_i = real[1] + real[3], imag[1] + imag[3]
    diff_r, diff_i = real[0] - real[2], imag[0] - imag[2]
    turn_r, turn_i = imag[1] - imag[3], real[3] - real[1]
    formed = (
        (even_r + odd_r, even_i + odd_i),
        (diff_r + turn_r, diff_i + turn_i),
        (even_r - odd_r, even_i - odd_i),
        (diff_r - turn_r, diff_i - turn_i),
    )
    for b, (re, im) in enumerate(formed):
        out_ref[:, b * GY : (b + 1) * GY] = (0.125 * (re * re + im * im)).astype(jnp.bfloat16)


def beamform(planes, grid_feed, piece, pieces):
    rows, feeds = planes.shape[1] // pieces, planes.shape[2]
    first = piece * rows // ROW_BLOCK
    place = (jnp.arange(feeds, dtype=jnp.int32)[:, None] == grid_feed[None, :]).astype(jnp.bfloat16)
    table = steering_table(GY, 1.0 / math.sqrt(GY))
    return pl.pallas_call(
        beam_kernel,
        grid=(rows // ROW_BLOCK,),
        in_specs=[
            pl.BlockSpec((2, ROW_BLOCK, feeds), lambda i: (0, first + i, 0)),
            pl.BlockSpec((feeds, feeds), lambda i: (0, 0)),
            pl.BlockSpec((2 * GY, 2 * GY), lambda i: (0, 0)),
        ],
        out_specs=pl.BlockSpec((ROW_BLOCK, feeds), lambda i: (i, 0)),
        out_shape=jax.ShapeDtypeStruct((rows, feeds), jnp.bfloat16),
        compiler_params=pltpu.CompilerParams(vmem_limit_bytes=40 * 2**20),
        cost_estimate=pl.CostEstimate(
            flops=2 * rows * feeds * (2 * feeds + 4 * GY),
            bytes_accessed=6 * rows * feeds,
            transcendentals=0,
        ),
    )(planes, place, table)


def sum_kernel(out_times, lag_ref, *refs):
    level_refs, (out_ref, select_ref, total_ref) = refs[:-3], refs[-3:]
    _, samples, channels, beams = level_refs[0].shape
    trials = lag_ref.shape[2]
    pieces = len(level_refs) // 2
    band = pl.program_id(0)
    per_piece = pl.num_programs(0) // pieces
    low = -0.5 / samples

    @pl.when(band == 0)
    def _():
        total_ref[...] = jnp.zeros_like(total_ref)

    for side in range(2):
        lag = lag_ref[side, 0].astype(jnp.float32)
        for step in range(-out_times[-1], samples - out_times[0]):
            block = jnp.where(lag == step, 1.0 + low, low).astype(jnp.bfloat16)
            for row, t in enumerate(out_times):
                s = t + step
                if 0 <= s < samples:
                    select_ref[
                        side,
                        row * trials : (row + 1) * trials,
                        s * channels : (s + 1) * channels,
                    ] = block
    for piece in range(pieces):

        @pl.when(band // per_piece == piece)
        def _():
            for side in range(2):
                levels = level_refs[2 * piece + side][...].reshape(samples * channels, beams)
                total_ref[...] += jnp.dot(
                    select_ref[side], levels, preferred_element_type=jnp.float32
                )

    out_ref[...] = total_ref[...].reshape(out_ref.shape).astype(out_ref.dtype)


def dedisperse(lags, level_pieces, out_times):
    _, bands, trials, channels = lags.shape
    per_piece, samples, _, beams = level_pieces[0].shape
    rows = len(out_times)

    def piece_spec(index):
        piece = index // 2
        return pl.BlockSpec(
            (1, samples, channels, beams),
            lambda b: (jnp.clip(b - piece * per_piece, 0, per_piece - 1), 0, 0, 0),
        )

    return pl.pallas_call(
        functools.partial(sum_kernel, out_times),
        grid=(bands,),
        in_specs=[pl.BlockSpec((2, 1, trials, channels), lambda b: (0, b, 0, 0))]
        + [piece_spec(index) for index in range(len(level_pieces))],
        out_specs=pl.BlockSpec((1, rows, trials, beams), lambda b: (b, 0, 0, 0)),
        out_shape=jax.ShapeDtypeStruct((bands, rows, trials, beams), jnp.bfloat16),
        scratch_shapes=[
            pltpu.VMEM((2, rows * trials, samples * channels), jnp.bfloat16),
            pltpu.VMEM((rows * trials, beams), jnp.float32),
        ],
        compiler_params=pltpu.CompilerParams(vmem_limit_bytes=48 * 2**20),
        cost_estimate=pl.CostEstimate(
            flops=4 * bands * rows * trials * samples * channels * beams,
            bytes_accessed=4 * bands * samples * channels * beams,
            transcendentals=0,
        ),
    )(lags, *level_pieces)


def regroup_lags(lags):
    size, me = lax.axis_size("freq"), lax.axis_index("freq")
    own = lax.dynamic_index_in_dim(lags, me, 0, keepdims=True)
    gathered = lax.dynamic_update_slice_in_dim(jnp.zeros_like(lags), own, me, 0)
    for shift in range(1, size):
        outgoing = lax.dynamic_index_in_dim(lags, (me + shift) % size, 0, keepdims=True)
        arrived = lax.ppermute(outgoing, "freq", [(i, (i + shift) % size) for i in range(size)])
        gathered = lax.dynamic_update_slice_in_dim(
            gathered, arrived, (me - shift) % size, 0
        )
    return gathered


def exchange(kept, axis_name, bit, dim):
    size = lax.axis_size(axis_name)
    mine = (lax.axis_index(axis_name) >> bit) & 1
    outgoing = lax.dynamic_index_in_dim(kept, 1 - mine, dim, keepdims=False).astype(jnp.bfloat16)
    own = lax.dynamic_index_in_dim(kept, mine, dim, keepdims=False)
    pairs = [(i, i ^ (1 << bit)) for i in range(size)]
    arrived = lax.ppermute(outgoing, axis_name, pairs)
    return own.astype(jnp.float32) + arrived.astype(jnp.float32)


def spread(part, band_bits, beam_bits, beams_first):
    def over_beam(a, lead):
        for bit in range(beam_bits):
            a = exchange(a, "beam", bit, lead + 2 + beam_bits - 1 - bit)
        return a

    def over_band(a):
        for bit in range(band_bits):
            a = exchange(a, "freq", bit, band_bits - 1 - bit)
        return a

    if beams_first:
        return over_band(over_beam(part, band_bits))
    return over_beam(over_band(part), 0)


def power_of_two(number):
    return number & (number - 1) == 0


def body(voltages, grid_feed, delays):
    bands, channels, samples = voltages.shape[0], voltages.shape[1], voltages.shape[2]
    feeds = voltages.shape[4]
    n_freq, n_beam = lax.axis_size("freq"), lax.axis_size("beam")
    fits = (
        channels % 128 == 0
        and delays.shape[0] == 1
        and delays.shape[2] % 128 == 0
        and bands == n_freq
        and power_of_two(n_freq)
        and power_of_two(n_beam)
        and (bands * channels * samples) % (2 * ROW_BLOCK) == 0
        and lax.axis_size("dm") == 2
        and bands % 2 == 0
        and samples % 4 == 0
        and feeds // n_beam % 128 == 0
    )
    if not fits:
        return regrouped_body(voltages, grid_feed, delays)

    trials = delays.shape[2]
    lags = delays[0].astype(jnp.bfloat16).reshape(n_freq, n_beam, channels, trials)
    lags = lax.dynamic_index_in_dim(lags, lax.axis_index("beam"), 1, keepdims=False)
    lags = jnp.transpose(lags, (0, 2, 1))
    lags = regroup_lags(lags)
    mine = lax.axis_index("dm").astype(jnp.bfloat16)
    lags = jnp.stack([lags - samples * mine, lags - samples * (1 - mine)])

    planes = jnp.transpose(voltages, (3, 0, 2, 1, 4)).reshape(2, -1, feeds)
    pieces = []
    for piece in range(2):
        own = beamform(planes, grid_feed, piece, 2)
        own = own.reshape(bands // 2, samples, channels, feeds)
        pieces += [own, lax.ppermute(own, "dm", [(0, 1), (1, 0)])]

    band_bits, beam_bits = n_freq.bit_length() - 1, n_beam.bit_length() - 1
    done = []
    for start in range(0, samples, 2):
        sums = dedisperse(lags, pieces, (start, start + 1))
        sums = sums.reshape(
            (2,) * band_bits + (2, trials) + (2,) * beam_bits + (feeds // n_beam,)
        )
        for row in range(2):
            part = lax.slice_in_dim(sums, row, row + 1, axis=band_bits)
            done.append(spread(part, band_bits, beam_bits, start + row > 0))
    done = jnp.concatenate(done, axis=0)
    return jnp.transpose(done, (1, 0, 2))[None] * (1.0 / math.sqrt(FREQS))


def solution(mesh):
    in_specs = (P(None, ("freq", "beam"), ("grp", "dm"), None, None), P(), P("freq", None, "dm"))
    out_specs = P("freq", "dm", "grp", "beam")
    return jax.shard_map(body, mesh=mesh, in_specs=in_specs, out_specs=out_specs, check_vma=False)
```
